128 devices in a mesh: dp: 1, cp: 128 (over z, y, x, core).
Axes of the slice: x: 4, y: 4, z: 4, core: 2. Of those that a mesh axis runs over, the one named last changes fastest.
Arguments:
- hidden: bfloat16 [16384, 3584], P(('dp', 'cp'))
- w_query: bfloat16 [6, 3584, 28, 128], replicated
- w_key: bfloat16 [6, 3584, 4, 128], replicated
- w_value: bfloat16 [6, 3584, 4, 128], replicated
- w_out: bfloat16 [6, 28, 128, 3584], replicated
Outputs:
- output: bfloat16 [16384, 3584], P(('dp', 'cp'))
All inputs are finite; a program needn't handle non-finite values.
Results may differ from the reference program's by a relative error of at most 0.0119431.
Values are sent between devices in bfloat16 or wider.
A program may use at most 1.5 GiB of HBM per device.

```python
import jax
import jax.numpy as jnp
from jax import lax

TOK_DEV = 128
NUM_CP = 128
D = 3584
HEADS = 28
KV_HEADS = 4
HEAD = 128
WINDOW = 1024
LAYERS = 6

SEQ_LEN = TOK_DEV * NUM_CP
GROUP_SIZE = HEADS // KV_HEADS
QUERY_BLOCK = min(64, TOK_DEV)
NUM_BLOCKS = SEQ_LEN // QUERY_BLOCK
EPS_NORM = 1e-6
NEG_BIG = -1e30


def setup_inputs(seed: int = 0, part: int = 0) -> dict:
    base_key = jax.random.key(seed)
    hidden_key = jax.random.fold_in(jax.random.fold_in(base_key, 1), part)
    weight_keys = jax.random.split(jax.random.fold_in(base_key, 2), 4)
    hidden = jax.random.normal(hidden_key, (SEQ_LEN, D), jnp.float32)
    w_query = jax.random.normal(weight_keys[0], (LAYERS, D, HEADS, HEAD), jnp.float32) * D ** -0.5
    w_key = jax.random.normal(weight_keys[1], (LAYERS, D, KV_HEADS, HEAD), jnp.float32) * D ** -0.5
    w_value = jax.random.normal(weight_keys[2], (LAYERS, D, KV_HEADS, HEAD), jnp.float32) * D ** -0.5
    w_out = jax.random.normal(weight_keys[3], (LAYERS, HEADS, HEAD, D), jnp.float32) * (HEADS * HEAD) ** -0.5
    return {
        "hidden": hidden.astype(jnp.bfloat16),
        "w_query": w_query.astype(jnp.bfloat16),
        "w_key": w_key.astype(jnp.bfloat16),
        "w_value": w_value.astype(jnp.bfloat16),
        "w_out": w_out.astype(jnp.bfloat16),
    }


def rms_normed(rows_in):
    widened = rows_in.astype(jnp.float32)
    return widened * lax.rsqrt(jnp.mean(widened * widened, axis=-1, keepdims=True) + EPS_NORM)


def project(normed, weight):
    flat = weight.reshape(weight.shape[0], weight.shape[1] * weight.shape[2])
    product = jnp.dot(normed, flat, preferred_element_type=jnp.float32)
    return product.astype(jnp.bfloat16).reshape(normed.shape[0], weight.shape[1], weight.shape[2])


def attend_block(q_block, key_rows, value_rows, query_pos, key_pos, windowed):
    grouped = q_block.astype(jnp.float32).reshape(QUERY_BLOCK, KV_HEADS, GROUP_SIZE, HEAD)
    scores = jnp.einsum("qhgd,khd->hgqk", grouped, key_rows) * HEAD ** -0.5
    allowed = (key_pos[None, :] <= query_pos[:, None]) & (key_pos[None, :] >= 0)
    if windowed:
        allowed = allowed & (key_pos[None, :] > query_pos[:, None] - WINDOW)
    scores = jnp.where(allowed, scores, NEG_BIG)
    row_max = jnp.max(scores, axis=-1, keepdims=True)
    weights = jnp.exp(scores - row_max)
    row_sum = jnp.sum(weights, axis=-1)
    rounded = weights.astype(jnp.bfloat16).astype(jnp.float32)
    attn_out = jnp.einsum("hgqk,khd->hgqd", rounded, value_rows) / row_sum[..., None]
    return jnp.transpose(attn_out, (2, 0, 1, 3)).reshape(QUERY_BLOCK, HEADS, HEAD).astype(jnp.bfloat16)


def attention_layer(hidden, weights, windowed):
    w_query, w_key, w_value, w_out = weights
    normed = rms_normed(hidden).astype(jnp.bfloat16)
    queries = project(normed, w_query)
    key_rows = project(normed, w_key).astype(jnp.float32)
    value_rows = project(normed, w_value).astype(jnp.float32)
    if windowed:
        zero_pad = jnp.zeros((WINDOW, KV_HEADS, HEAD), jnp.float32)
        key_rows = jnp.concatenate([zero_pad, key_rows], axis=0)
        value_rows = jnp.concatenate([zero_pad, value_rows], axis=0)

    def one_block(block_idx):
        start_row = block_idx * QUERY_BLOCK
        q_block = lax.dynamic_slice_in_dim(queries, start_row, QUERY_BLOCK)
        query_pos = start_row + jnp.arange(QUERY_BLOCK)
        if windowed:
            key_span = WINDOW + QUERY_BLOCK
            key_blk = lax.dynamic_slice_in_dim(key_rows, start_row, key_span)
            value_blk = lax.dynamic_slice_in_dim(value_rows, start_row, key_span)
            key_pos = start_row - WINDOW + jnp.arange(key_span)
        else:
            key_blk = key_rows
            value_blk = value_rows
            key_pos = jnp.arange(SEQ_LEN)
        return attend_block(q_block, key_blk, value_blk, query_pos, key_pos, windowed)

    attn_out = lax.map(one_block, jnp.arange(NUM_BLOCKS)).reshape(SEQ_LEN, HEADS * HEAD)
    update = jnp.dot(attn_out, w_out.reshape(HEADS * HEAD, D), preferred_element_type=jnp.float32)
    return (hidden.astype(jnp.float32) + rms_normed(update)).astype(jnp.bfloat16)


def output_order(hidden):
    halves = hidden.reshape(2, NUM_CP, TOK_DEV // 2, D)
    return jnp.stack([halves[0], halves[1, ::-1]], axis=1).reshape(SEQ_LEN, D)


def reference(hidden, w_query, w_key, w_value, w_out):
    def local_step(state_in, weights):
        return attention_layer(state_in, weights, True), None

    stacked = (w_query[:LAYERS - 1], w_key[:LAYERS - 1], w_value[:LAYERS - 1], w_out[:LAYERS - 1])
    hidden = lax.scan(local_step, hidden, stacked)[0]
    last_weights = (w_query[LAYERS - 1], w_key[LAYERS - 1], w_value[LAYERS - 1], w_out[LAYERS - 1])
    hidden = attention_layer(hidden, last_weights, False)
    return output_order(hidden)
```

```python
import functools

import jax
import jax.numpy as jnp
from jax import lax
from jax.experimental import pallas as pl
from jax.experimental.pallas import tpu as pltpu
from jax.sharding import PartitionSpec as P

WINDOW = 1024
EPS_NORM = 1e-6
NEG_BIG = -1e30
HEAD = 128
ROWS = 128
RING_X = 4
PIECES_HALF = 2
LOG2E = 1.4426950408889634
VMEM_BYTES = 66_000_000
MESH = pl.DeviceIdType.MESH


def rms_normed(rows_in):
    widened = rows_in.astype(jnp.float32)
    return widened * lax.rsqrt(jnp.mean(widened * widened, axis=-1, keepdims=True) + EPS_NORM)


def window_kernel(cfg, x_in, wkv, wq, wo, x_ref, n_ref, o_ref, a_ref, ssq_ref, q_ref, kv_ref, s_ref, p_ref, ring,
                  ring_sem, ici_recv, d2d_recv, send_sem, d2d_send):
    layers, kvh, group, width, num_dev = cfg
    hq = kvh * group
    scale2 = HEAD ** -0.5 * LOG2E
    half = width // 256
    chunks_kv, chunks_q, chunks_o = kvh, hq // 2, half
    chunks = chunks_kv + chunks_q + chunks_o
    slots = chunks_kv + chunks_q
    total_chunks = layers * chunks
    num_chips = num_dev // 2
    pieces = kvh
    piece_cut = kvh // 2
    rounds = 7
    per_round = chunks_q // rounds

    dev = lax.axis_index("cp")
    chip = lax.div(dev, 2)
    core = lax.rem(dev, 2)
    col = lax.rem(chip, RING_X)
    partner = dev + 1 - 2 * core
    right = dev + 2 * (lax.rem(col + 1, RING_X) - col)
    left = dev + 2 * (lax.rem(col + RING_X - 1, RING_X) - col)
    upper = dev + 2 * RING_X
    has_up = chip + RING_X < num_chips

    def has(dist):
        return chip >= dist

    def weight_copies(layer, chunk, slot, start):
        def go(src0, src1):
            for j, src in enumerate((src0, src1)):
                copy = pltpu.make_async_copy(src, ring.at[slot, j], ring_sem.at[slot, j])
                copy.start() if start else copy.wait()

        if not start:
            go(wkv.at[0, 0], wkv.at[0, 1])
            return

        @pl.when(chunk < chunks_kv)
        def _():
            go(wkv.at[layer, 2 * chunk], wkv.at[layer, 2 * chunk + 1])

        @pl.when((chunk >= chunks_kv) & (chunk < slots))
        def _():
            idx = chunk - chunks_kv
            go(wq.at[layer, 2 * idx], wq.at[layer, 2 * idx + 1])

        @pl.when(chunk >= slots)
        def _():
            off = pl.multiple_of((chunk - slots) * 256, 256)
            go(wo.at[layer, :, pl.ds(off, 128)], wo.at[layer, :, pl.ds(off + 128, 128)])

    def slot_of(layer, chunk):
        return lax.rem(layer * chunks + chunk, slots)

    def refill(layer, chunk):
        nxt = chunk + slots
        layer_nxt = layer + lax.div(nxt, chunks)
        chunk_nxt = lax.rem(nxt, chunks)

        @pl.when(layer * chunks + nxt < total_chunks)
        def _():
            weight_copies(layer_nxt, chunk_nxt, slot_of(layer, chunk), True)

    def project(lhs_ref, layer, chunk):
        slot = slot_of(layer, chunk)
        weight_copies(layer, chunk, slot, False)
        rhs = jnp.concatenate([ring[slot, 0], ring[slot, 1]], axis=1)
        out = jnp.dot(lhs_ref[...], rhs, preferred_element_type=jnp.float32)
        return out

    def ici(layer, src_slot, dist, piece, kind, target):
        return pltpu.make_async_remote_copy(
            src_ref=kv_ref.at[layer, src_slot, piece], dst_ref=kv_ref.at[layer, 2 * dist, piece],
            send_sem=send_sem.at[kind, piece], recv_sem=ici_recv.at[layer, dist - 1, piece],
            device_id={"cp": target}, device_id_type=MESH)

    def up_copy(layer, piece):
        return ici(layer, 0, 4, piece, 0, upper)

    def right_own(layer, piece):
        return ici(layer, 0, 1, piece, 1, right)

    def right_prev(layer, piece):
        return ici(layer, 8, 1, piece, 1, right)

    def left_own(layer, piece):
        return ici(layer, 0, 3, piece, 2, left)

    def left_prev(layer, piece):
        return ici(layer, 8, 3, piece, 2, left)

    def relay_right(layer, piece):
        return ici(layer, 2, 2, piece, 3, right)

    def relay_left(layer, piece):
        return ici(layer, 6, 2, piece, 4, left)

    def d2d(layer, idx):
        dist = idx + core
        return pltpu.make_async_remote_copy(
            src_ref=kv_ref.at[layer, 2 * dist], dst_ref=kv_ref.at[layer, 2 * dist + 1 - 2 * core],
            send_sem=d2d_send.at[idx], recv_sem=d2d_recv.at[layer, idx],
            device_id={"cp": partner}, device_id_type=MESH)

    def recv_ici(layer, dist, piece):
        ici(layer, 0, dist, piece, 0, dev).wait_recv()

    def recv_d2d(layer, idx):
        dist = idx + 1 - core
        pltpu.make_async_remote_copy(
            src_ref=kv_ref.at[layer, 0], dst_ref=kv_ref.at[layer, 2 * dist - 1 + 2 * core],
            send_sem=d2d_send.at[idx], recv_sem=d2d_recv.at[layer, idx],
            device_id={"cp": partner}, device_id_type=MESH).wait_recv()

    goes_right = (col < RING_X - 1) | has(4)
    relays_right_all = (col == RING_X - 2) & has(1)
    relays_right_half = (col < RING_X - 2) & has(1)
    relays_left_all = (col == 1) & has(3)
    relays_left_half = (col > 1) & has(3)

    def does_relay_right(piece):
        return relays_right_all | (relays_right_half & (piece < piece_cut))

    def does_relay_left(piece):
        return relays_left_all | (relays_left_half & (piece >= piece_cut))

    def send_own(layer):
        def body(piece, carry):
            @pl.when(has_up)
            def _():
                up_copy(layer, piece).start()

            @pl.when(col < RING_X - 1)
            def _():
                right_own(layer, piece).start()

            @pl.when(col == 0)
            def _():
                left_own(layer, piece).start()

            return carry

        lax.fori_loop(0, pieces, body, 0)

        @pl.when(core == 0)
        def _():
            d2d(layer, 0).start()

    def forward_d2d(layer, dist, cond):
        @pl.when(cond & has(dist) & (dist - core < 4))
        def _():
            d2d(layer, dist - core).start()

    def comm_round(layer, k):
        in_a = (k < pieces)
        p_a = jnp.minimum(k, pieces - 1)

        @pl.when(in_a & has(4))
        def _():
            recv_ici(layer, 4, p_a)

            @pl.when(col >= 1)
            def _():
                left_prev(layer, p_a).start()

            @pl.when(col == RING_X - 1)
            def _():
                right_prev(layer, p_a).start()

        forward_d2d(layer, 4, k == pieces - 1)

        in_b = (k >= 1) & (k < pieces + 1)
        p_b = jnp.clip(k - 1, 0, pieces - 1)

        @pl.when(in_b & has(1))
        def _():
            recv_ici(layer, 1, p_b)

            @pl.when(does_relay_right(p_b))
            def _():
                relay_right(layer, p_b).start()

        forward_d2d(layer, 1, k == pieces)

        in_c = (k >= 2) & (k < pieces + 2)
        p_c = jnp.clip(k - 2, 0, pieces - 1)

        @pl.when(in_c & has(3))
        def _():
            recv_ici(layer, 3, p_c)

            @pl.when(does_relay_left(p_c))
            def _():
                relay_left(layer, p_c).start()

        forward_d2d(layer, 3, k == pieces + 1)

    def comm_last(layer):
        @pl.when(has(2))
        def _():
            def body(piece, carry):
                recv_ici(layer, 2, piece)
                return carry

            lax.fori_loop(0, pieces, body, 0)

        forward_d2d(layer, 2, True)

    def comm_join(layer):
        def body(idx, carry):
            @pl.when(has(idx + 1 - core))
            def _():
                recv_d2d(layer, idx)

            return carry

        lax.fori_loop(0, 4, body, 0)

    def comm_drain(layer):
        def body(piece, carry):
            @pl.when(has_up)
            def _():
                up_copy(layer, piece).wait_send()

            @pl.when(goes_right)
            def _():
                right_own(layer, piece).wait_send()

            @pl.when((col == 0) | has(4))
            def _():
                left_own(layer, piece).wait_send()

            @pl.when(does_relay_right(piece))
            def _():
                relay_right(layer, piece).wait_send()

            @pl.when(does_relay_left(piece))
            def _():
                relay_left(layer, piece).wait_send()

            return carry

        lax.fori_loop(0, pieces, body, 0)

        def body_d2d(idx, carry):
            @pl.when(has(idx + core))
            def _():
                d2d(layer, idx).wait_send()

            return carry

        lax.fori_loop(0, 4, body_d2d, 0)

    def prime(chunk, carry):
        weight_copies(0, chunk, chunk, True)
        return carry

    lax.fori_loop(0, slots, prime, 0)
    x_ref[...] = x_in[...]

    def zero_slots(idx, carry):
        @pl.when(dev < idx)
        def _():
            for layer in range(layers):
                kv_ref[layer, idx] = jnp.zeros(kv_ref.shape[2:], kv_ref.dtype)

        return carry

    lax.fori_loop(1, 9, zero_slots, 0)

    def layer_body(layer, carry):
        part = jnp.zeros((ROWS, 128), jnp.float32)
        for c in range(half):
            xv = x_ref[:, c * 256:(c + 1) * 256].astype(jnp.float32)
            sq = xv * xv
            part = part + sq[:, :128] + sq[:, 128:]
        rstd = lax.rsqrt(jnp.sum(part, axis=1, keepdims=True) * (1.0 / width) + EPS_NORM)
        for c in range(half):
            xv = x_ref[:, c * 256:(c + 1) * 256].astype(jnp.float32)
            n_ref[:, c * 256:(c + 1) * 256] = (xv * rstd).astype(jnp.bfloat16)

        def k_body(c, carry):
            out = project(n_ref, layer, c)
            kv_ref[layer, 0, 2 * c, 0] = out[:, :128].astype(jnp.bfloat16)
            kv_ref[layer, 0, 2 * c + 1, 0] = out[:, 128:].astype(jnp.bfloat16)
            refill(layer, c)
            return carry

        lax.fori_loop(0, chunks_kv // 2, k_body, 0)

        def v_body(c, carry):
            out = project(n_ref, layer, chunks_kv // 2 + c)
            kv_ref[layer, 0, 2 * c, 1] = out[:, :128].T.astype(jnp.bfloat16)
            kv_ref[layer, 0, 2 * c + 1, 1] = out[:, 128:].T.astype(jnp.bfloat16)
            refill(layer, chunks_kv // 2 + c)
            return carry

        lax.fori_loop(0, chunks_kv // 2, v_body, 0)
        send_own(layer)

        def q_round(k, carry):
            def q_body(j, carry):
                idx = k * per_round + j
                out = project(n_ref, layer, chunks_kv + idx)
                q_ref[2 * idx] = out[:, :128].T.astype(jnp.bfloat16)
                q_ref[2 * idx + 1] = out[:, 128:].T.astype(jnp.bfloat16)
                refill(layer, chunks_kv + idx)
                return carry

            lax.fori_loop(0, per_round, q_body, 0)
            comm_round(layer, k)
            return carry

        lax.fori_loop(0, rounds, q_round, 0)
        comm_last(layer)
        comm_join(layer)

        key_iota = lax.broadcasted_iota(jnp.int32, (128, 128), 0)
        row_iota = lax.broadcasted_iota(jnp.int32, (128, 128), 1)
        causal = key_iota <= row_iota

        def attend(g, carry):
            for t0 in range(0, group, 2):
                heads = list(range(t0, min(t0 + 2, group)))
                cols = 128 * len(heads)
                q_t = jnp.concatenate([q_ref[g * group + h] for h in heads], axis=1) if len(heads) > 1 \
                    else q_ref[g * group + heads[0]]
                mask = jnp.concatenate([causal] * len(heads), axis=1)
                best = jnp.full((8, cols), NEG_BIG, jnp.float32)
                for b in range(9):
                    s = jnp.dot(kv_ref[layer, b, g, 0], q_t, preferred_element_type=jnp.float32)
                    if b == 0:
                        s = jnp.where(mask, s, NEG_BIG)
                    if b == 8:
                        s = jnp.where(mask, NEG_BIG, s)
                    s_ref[t0 // 2, b, :, :cols] = s
                    top = jnp.max(s.reshape(16, 8, cols), axis=0)
                    if b > 0:
                        top = jnp.where(dev >= b, top, NEG_BIG)
                    best = jnp.maximum(best, top)
                m2 = jnp.max(best, axis=0, keepdims=True) * scale2
                total = jnp.zeros((8, cols), jnp.float32)
                for b in range(9):
                    shift = m2 if b == 0 else jnp.where(dev >= b, m2, -NEG_BIG)
                    e = jnp.exp2(s_ref[t0 // 2, b, :, :cols] * scale2 - shift)
                    total = total + jnp.sum(e.reshape(16, 8, cols), axis=0)
                    p_ref[t0 // 2, b * 128:(b + 1) * 128, :cols] = e.astype(jnp.bfloat16)
                v_t = jnp.concatenate([kv_ref[layer, b, g, 1] for b in range(9)], axis=1)
                acc = jnp.dot(v_t, p_ref[t0 // 2, :, :cols], preferred_element_type=jnp.float32)
                acc = acc / jnp.sum(total, axis=0, keepdims=True)
                for j, h in enumerate(heads):
                    o_ref[g * group + h] = acc[:, 128 * j:128 * (j + 1)].T.astype(jnp.bfloat16)
            return carry

        lax.fori_loop(0, kvh, attend, 0)

        ssq_ref[...] = jnp.zeros_like(ssq_ref)
        for h in range(hq):
            n_ref_o = o_ref[h]
            a_ref[:, h * 128:(h + 1) * 128] = n_ref_o

        def o_body(c, carry):
            out = project(a_ref, layer, slots + c)
            u_ref = s_ref
            u_ref[lax.div(c, 9), lax.rem(c, 9)] = out
            sq = out * out
            ssq_ref[...] += sq[:, :128] + sq[:, 128:]
            refill(layer, slots + c)
            return carry

        lax.fori_loop(0, chunks_o, o_body, 0)
        rstd_a = lax.rsqrt(jnp.sum(ssq_ref[...], axis=1, keepdims=True) * (1.0 / width) + EPS_NORM)
        for c in range(half):
            xv = x_ref[:, c * 256:(c + 1) * 256].astype(jnp.float32)
            x_ref[:, c * 256:(c + 1) * 256] = (xv + s_ref[c // 9, c % 9] * rstd_a).astype(jnp.bfloat16)
        comm_drain(layer)
        return carry

    lax.fori_loop(0, layers, layer_body, 0)


def window_layers(hidden, wkv, wq, wo, layers, num_dev):
    width = hidden.shape[1]
    hq = wq.shape[1]
    kvh = wkv.shape[1] // 2
    group = hq // kvh
    cfg = (layers, kvh, group, width, num_dev)
    slots = kvh + hq // 2
    flops = layers * 2 * ROWS * width * (2 * hq + 2 * kvh) * HEAD
    bf16 = jnp.bfloat16
    return pl.pallas_call(
        functools.partial(window_kernel, cfg),
        out_shape=jax.ShapeDtypeStruct((ROWS, width), bf16),
        in_specs=[pl.BlockSpec(memory_space=pltpu.VMEM)] + [pl.BlockSpec(memory_space=pl.ANY)] * 3,
        out_specs=pl.BlockSpec(memory_space=pltpu.VMEM),
        scratch_shapes=[
            pltpu.VMEM((ROWS, width), bf16),
            pltpu.VMEM((hq, ROWS, HEAD), bf16),
            pltpu.VMEM((ROWS, hq * HEAD), bf16),
            pltpu.VMEM((ROWS, 128), jnp.float32),
            pltpu.VMEM((hq, HEAD, ROWS), bf16),
            pltpu.VMEM((layers, 9, kvh, 2, 128, 128), bf16),
            pltpu.VMEM(((group + 1) // 2, 9, 128, 256), jnp.float32),
            pltpu.VMEM(((group + 1) // 2, 9 * 128, 256), bf16),
            pltpu.VMEM((slots, 2, width, 128), bf16),
            pltpu.SemaphoreType.DMA((slots, 2)),
            pltpu.SemaphoreType.DMA((layers, 4, kvh)),
            pltpu.SemaphoreType.DMA((layers, 4)),
            pltpu.SemaphoreType.DMA((5, kvh)),
            pltpu.SemaphoreType.DMA((4,)),
        ],
        compiler_params=pltpu.CompilerParams(has_side_effects=True, vmem_limit_bytes=VMEM_BYTES),
        cost_estimate=pl.CostEstimate(flops=flops, bytes_accessed=layers * (wkv[0].size + wq[0].size + wo[0].size) * 2,
                                      transcendentals=0),
        name="window_layers",
    )(hidden, wkv, wq, wo)


def output_owner(block_idx, num_dev):
    return block_idx if block_idx < num_dev else 2 * num_dev - 1 - block_idx


def to_output_layout(hidden, dev_rank, num_dev):
    block_len = hidden.shape[0] // 2
    even_pairs = [(source, output_owner(2 * source, num_dev)) for source in range(num_dev)]
    odd_pairs = [(source, output_owner(2 * source + 1, num_dev)) for source in range(num_dev)]
    from_even = lax.ppermute(hidden[:block_len], "cp", even_pairs)
    from_odd = lax.ppermute(hidden[block_len:], "cp", odd_pairs)
    is_even = dev_rank % 2 == 0
    lead_rows = jnp.where(is_even, from_even, from_odd)
    trail_rows = jnp.where(is_even, from_odd, from_even)
    return jnp.concatenate([lead_rows, trail_rows], axis=0)


KEY_TILE = 512


def causal_kernel(cfg, q_in, kv_hbm, o_ref, qt_ref, m_ref, l_ref, acc_ref, buf, sem):
    kvh, group, num_dev = cfg
    scale2 = HEAD ** -0.5 * LOG2E
    dev = lax.axis_index("cp")
    cols = group * 64
    for half in range(2):
        for h in range(kvh * group):
            blk = q_in[half * 64:(half + 1) * 64, h * 128:(h + 1) * 128].astype(jnp.float32)
            qt_ref[half, h // group, :, (h % group) * 64:(h % group + 1) * 64] = blk.T.astype(jnp.bfloat16)
    m_ref[...] = jnp.full_like(m_ref, NEG_BIG)
    l_ref[...] = jnp.zeros_like(l_ref)
    acc_ref[...] = jnp.zeros_like(acc_ref)
    blocks = (dev, 2 * num_dev - 1 - dev)
    tiles = [lax.div((b + 1) * 64 + KEY_TILE - 1, KEY_TILE) for b in blocks]

    def fetch(t, slot):
        return pltpu.make_async_copy(kv_hbm.at[pl.ds(pl.multiple_of(t * KEY_TILE, KEY_TILE), KEY_TILE)], buf.at[slot],
                                     sem.at[slot])

    fetch(0, 0).start()

    def step(half, t, slot):
        key_pos = t * KEY_TILE + lax.broadcasted_iota(jnp.int32, (KEY_TILE, 64), 0)
        row_pos = blocks[half] * 64 + lax.broadcasted_iota(jnp.int32, (KEY_TILE, 64), 1)
        allowed = (key_pos - row_pos <= 0)
        bias1 = jnp.where(allowed, 0.0, NEG_BIG)
        bias = jnp.concatenate([bias1] * group, axis=1)
        for g in range(kvh):
            k = buf[slot, :, g * 128:(g + 1) * 128]
            v_t = buf[slot, :, (kvh + g) * 128:(kvh + g + 1) * 128].T
            s = jnp.dot(k, qt_ref[half, g], preferred_element_type=jnp.float32) + bias
            m_old = m_ref[half, g]
            m_new = jnp.maximum(m_old, jnp.max(s, axis=0, keepdims=True))
            alpha = jnp.exp2((m_old - m_new) * scale2)
            e = jnp.exp2((s - m_new) * scale2)
            l_ref[half, g] = l_ref[half, g] * alpha + jnp.sum(e, axis=0, keepdims=True)
            acc_ref[half, g] = acc_ref[half, g] * alpha + jnp.dot(v_t, e.astype(jnp.bfloat16),
                                                                  preferred_element_type=jnp.float32)
            m_ref[half, g] = m_new

    def body(t, carry):
        slot = lax.rem(t, 2)

        @pl.when(t + 1 < tiles[1])
        def _():
            fetch(t + 1, 1 - slot).start()

        fetch(t, slot).wait()
        step(1, t, slot)

        @pl.when(t < tiles[0])
        def _():
            step(0, t, slot)

        return carry

    lax.fori_loop(0, tiles[1], body, 0)
    for half in range(2):
        for g in range(kvh):
            out = acc_ref[half, g] / l_ref[half, g]
            for j in range(group):
                h = g * group + j
                o_ref[half * 64:(half + 1) * 64, h * 128:(h + 1) * 128] = \
                    out[:, j * 64:(j + 1) * 64].T.astype(jnp.bfloat16)


def causal_attention(queries, kv_all, kvh, num_dev):
    rows, width = queries.shape
    group = width // HEAD // kvh
    return pl.pallas_call(
        functools.partial(causal_kernel, (kvh, group, num_dev)),
        out_shape=jax.ShapeDtypeStruct((rows, width), jnp.bfloat16),
        in_specs=[pl.BlockSpec(memory_space=pltpu.VMEM), pl.BlockSpec(memory_space=pl.ANY)],
        out_specs=pl.BlockSpec(memory_space=pltpu.VMEM),
        scratch_shapes=[
            pltpu.VMEM((2, kvh, HEAD, group * 64), jnp.bfloat16),
            pltpu.VMEM((2, kvh, 1, group * 64), jnp.float32),
            pltpu.VMEM((2, kvh, 1, group * 64), jnp.float32),
            pltpu.VMEM((2, kvh, HEAD, group * 64), jnp.float32),
            pltpu.VMEM((2, KEY_TILE, 2 * kvh * HEAD), jnp.bfloat16),
            pltpu.SemaphoreType.DMA((2,)),
        ],
        compiler_params=pltpu.CompilerParams(vmem_limit_bytes=VMEM_BYTES),
        cost_estimate=pl.CostEstimate(flops=4 * rows * width * kv_all.shape[0] // 2, bytes_accessed=kv_all.size * 2,
                                      transcendentals=0),
        name="causal_attention",
    )(queries, kv_all)


def solution(mesh):
    num_dev = mesh.shape["cp"]

    def per_device(hidden, w_query, w_key, w_value, w_out):
        dev_rank = lax.axis_index("cp")
        layers, width, hq, _ = w_query.shape
        kvh = w_key.shape[2]
        last = layers - 1
        wq = jnp.transpose(w_query, (0, 2, 1, 3))
        wkv = jnp.transpose(jnp.concatenate([w_key, w_value], axis=2), (0, 2, 1, 3))
        wo = w_out.reshape(layers, hq * HEAD, width)
        hidden = window_layers(hidden, wkv, wq, wo, last, num_dev)

        normed = rms_normed(hidden).astype(jnp.bfloat16)
        kv_own = jnp.einsum("td,hde->the", normed, wkv[last], preferred_element_type=jnp.float32)
        kv_own = kv_own.astype(jnp.bfloat16).reshape(ROWS, 2 * kvh * HEAD)
        kv_all = lax.all_gather(kv_own, "cp", tiled=True)
        hidden = to_output_layout(hidden, dev_rank, num_dev)
        normed = rms_normed(hidden).astype(jnp.bfloat16)
        queries = jnp.einsum("td,hde->the", normed, wq[last], preferred_element_type=jnp.float32)
        queries = queries.astype(jnp.bfloat16).reshape(ROWS, hq * HEAD)
        attn = causal_attention(queries, kv_all, kvh, num_dev)
        update = jnp.dot(attn, wo[last], preferred_element_type=jnp.float32)
        return (hidden.astype(jnp.float32) + rms_normed(update)).astype(jnp.bfloat16)

    row_spec = P(("dp", "cp"), None)
    return jax.shard_map(per_device, mesh=mesh, in_specs=(row_spec, P(), P(), P(), P()), out_specs=row_spec, check_vma=False)
```
